32 devices in a mesh: pw: 2 (over x), pair: 16 (over z, y, core).
Axes of the slice: x: 2, y: 2, z: 4, core: 2. Of those that a mesh axis runs over, the one named last changes fastest.
Arguments:
- valence_pairs: bfloat16 [64, 64, 8192], P('pair', None, 'pw'), may hold values from -0.59765625 to 0.59765625
- conduction_pairs: bfloat16 [16, 256, 8192], P('pair', None, 'pw'), may hold values from -0.59765625 to 0.59765625
- screening: float32 [8192], P('pw'), may hold values from 0.1 to 2
Outputs:
- kernel: float32 [64, 16, 64, 256], P('pair', None, 'pw')
The draws below stay inside these ranges and needn't reach their ends.
All inputs are finite; a program needn't handle non-finite values.
Results may differ from the reference program's by a relative error of at most 0.0029.
Values may be sent and summed in bfloat16 or wider, within the bound.
A program may use at most 128 MiB of HBM per device.

```python
import math
import jax
import jax.numpy as jnp
from jax import lax

V = 64
C = 256
G = 8192
CS = 16


def raised(entries, own_key, source, target, shards_of, factor):
    owner, partner = [(jnp.arange(entries.shape[dim]) // (entries.shape[dim] // shards_of)).reshape([-1 if axis == dim else 1 for axis in range(entries.ndim)]) for dim in (source, target)]
    chosen = jax.random.permutation(own_key, shards_of)[partner]
    strong = (owner == chosen) | (owner == (partner + shards_of // 2) % shards_of)
    return jnp.where(strong, factor * entries, entries)


def levels(stream_key, shape, shards, least, largest):
    gain = 1.0
    for dim, parts in shards:
        draws = jax.random.uniform(jax.random.fold_in(jax.random.fold_in(stream_key, 6), dim), (parts,), jnp.float32, least / len(shards), largest / len(shards))
        gain = gain * jnp.repeat(jnp.exp(draws), shape[dim] // parts).reshape((-1,) + (1,) * (len(shape) - 1 - dim))
    return gain


def gaussian(rng, dims, spread, most, pieces=(), held_as=jnp.bfloat16):
    array = jax.random.normal(rng, dims, jnp.float32) * spread
    if len(pieces) > 0:
        array = levels(rng, dims, pieces, -0.22, 0.18) * array
    return jnp.clip(array, min=-most, max=most).astype(held_as)


def heavy_noise(key, dims, scale, limit, split, heavy, held_as=jnp.bfloat16):
    entries = scale * jax.random.normal(key, dims, jnp.float32)
    if split:
        entries = entries * levels(key, dims, split, -0.22, 0.18)
    return jnp.clip(raised(entries, jax.random.fold_in(key, 3), *heavy), -limit, limit).astype(held_as)


def setup_inputs(seed: int = 0) -> dict:
    streams_of = jax.random.split(jax.random.key(seed), 4)
    valence_pairs = heavy_noise(streams_of[0], (V, V, G), 0.1, 0.59765625, ((0, 16), (2, 2)), (2, 1, 2, 2.0))
    conduction_pairs = gaussian(streams_of[1], (CS, C, G), 0.1, 0.59765625, ((0, 16), (2, 2)))
    screening = jnp.clip(jnp.exp(math.log(2.0) - 2.9957323 * jax.random.uniform(streams_of[2], (G,), jnp.float32) ** levels(streams_of[2], (G,), ((0, 2),), -0.2, 0.2)), 0.1, 2.0)
    return {"valence_pairs": valence_pairs, "conduction_pairs": conduction_pairs, "screening": screening}


def reference(valence_pairs, conduction_pairs, screening):
    screened = (valence_pairs.astype(jnp.float32) * screening[None, None, :]).astype(jnp.bfloat16)
    left = screened.astype(jnp.float32).reshape(V * V, G)
    right = conduction_pairs.astype(jnp.float32).reshape(CS * C, G)
    product = lax.dot_general(left, right, (((1,), (1,)), ((), ())), preferred_element_type=jnp.float32)
    return product.reshape(V, V, CS, C).transpose(0, 2, 1, 3)
```

```python
import functools

import jax
import jax.numpy as jnp
from jax import lax
from jax.experimental import pallas as pl
from jax.experimental.pallas import tpu as pltpu
from jax.sharding import PartitionSpec as P

MESH = pl.DeviceIdType.MESH
SIDE = 4
CHUNKS = 4


def contract(piece, flat_right, band_dev, conduction):
    first, second, width = piece.shape
    product = lax.dot_general(
        piece.reshape(first * second, width),
        flat_right,
        (((1,), (1,)), ((), ())),
        preferred_element_type=jnp.float32,
    )
    return product.reshape(first, second, band_dev, conduction)


def general_body(valence_pairs, conduction_pairs, screening):
    screened = (valence_pairs.astype(jnp.float32) * screening[None, None, :]).astype(jnp.bfloat16)
    band_dev, conduction, plane_dev = conduction_pairs.shape
    flat_local = conduction_pairs.reshape(band_dev * conduction, plane_dev)
    partial_value = contract(
        lax.all_gather(screened, "pair", axis=0, tiled=True), flat_local, band_dev, conduction
    )
    terms = lax.psum_scatter(partial_value, "pw", scatter_dimension=1, tiled=True)
    owned = lax.all_to_all(terms, "pair", split_axis=0, concat_axis=2, tiled=True)
    return owned.transpose(0, 2, 1, 3)


def flip(bit, by):
    return bit + by - 2 * bit * by


def grid_kernel(
    val, con, scr_row, out, raw, scr, bb, acc, xs, xr, zs, zr,
    loc, a1s, a1r, a2s, a2r, a3s, a3r, b1s, b1r, b2s, b2r, b3s, b3r, xss, xsr, zss, zsr,
):
    me, x = lax.axis_index("pair"), lax.axis_index("pw")
    core, y, zl, zh = me % 2, (me // 2) % 2, (me // 4) % 2, me // 8
    rows, depth = val.shape
    cols = con.shape[0]
    half = out.shape[2]
    step = rows // CHUNKS
    cstep = cols // CHUNKS

    def at(fc, fy, fl, fh):
        return (x, flip(core, fc) + 2 * flip(y, fy) + 4 * flip(zl, fl) + 8 * flip(zh, fh))

    def remote(src, dst, s, r, dev):
        return pltpu.make_async_remote_copy(
            src_ref=src, dst_ref=dst, send_sem=s, recv_sem=r, device_id=dev, device_id_type=MESH
        )

    def arows(k):
        return pl.ds(pl.multiple_of(k * step, step), step)

    def brows(k):
        return pl.ds(pl.multiple_of(k * cstep, cstep), cstep)

    sibling, beside, near, far = at(1, 0, 0, 0), at(0, 1, 0, 0), at(0, 0, 1, 0), at(0, 0, 0, 1)
    a1 = remote(val, raw.at[1], a1s.at[0], a1r.at[0], sibling)
    b1 = remote(con, bb.at[1], b1s.at[0], b1r.at[0], beside)

    def a2(k):
        return remote(val.at[arows(k)], raw.at[2, arows(k)], a2s.at[k], a2r.at[k], near)

    def b2(k):
        return remote(con.at[brows(k)], bb.at[2, brows(k)], b2s.at[k], b2r.at[k], far)

    def a3(k):
        return remote(raw.at[2, arows(k)], raw.at[3, arows(k)], a3s.at[k], a3r.at[k], sibling)

    def b3(k):
        return remote(bb.at[2, brows(k)], bb.at[3, brows(k)], b3s.at[k], b3r.at[k], beside)

    def xcopy(t):
        return remote(xs.at[t], xr.at[t], xss.at[t], xsr.at[t], (1 - x, me))

    def zcopy(t):
        a = t // SIDE
        return remote(zs.at[t], zr.at[t], zss.at[t], zsr.at[t], at(a % 2, 0, a // 2, 0))

    def each(n, fn, lo=0):
        def run(k, carry):
            fn(k)
            return carry
        lax.fori_loop(lo, n, run, 0)

    barrier = pltpu.get_barrier_semaphore()
    greeted = (sibling, beside, near, far, at(1, 0, 1, 0), (1 - x, me))
    for dev in greeted:
        pl.semaphore_signal(barrier, inc=1, device_id=dev, device_id_type=MESH)
    own_a = pltpu.make_async_copy(val, raw.at[0], loc.at[0])
    own_b = pltpu.make_async_copy(con, bb.at[0], loc.at[1])
    own_a.start()
    own_b.start()
    pl.semaphore_wait(barrier, len(greeted))

    end = zl == zh

    @pl.when(end)
    def _():
        each(CHUNKS, lambda k: a2(k).start())
        each(CHUNKS, lambda k: b2(k).start())

    @pl.when(jnp.logical_not(end))
    def _():
        each(CHUNKS, lambda k: b2(k).start())

    b1.start()
    a1.start()

    def screen(a):
        def part(i):
            r = pl.ds(pl.multiple_of(i * 16, 16), 16)
            scr[a, r, :] = (raw[a, r, :].astype(jnp.float32) * scr_row[...]).astype(jnp.bfloat16)
        each(rows // 16, part)

    kc = min(depth, 1024)
    vb, w = acc.shape[1], acc.shape[2]

    def owned_c(a, b):
        return flip(core, a % 2) + 2 * flip(y, b % 2) + 4 * flip(zl, a // 2) + 8 * flip(zh, b // 2)

    def group(lo, hi, b):
        def mm(a):
            t = a * SIDE + b
            acc[t] = jnp.zeros((vb, w, cols), jnp.float32)

            def kk(k):
                ks = pl.ds(pl.multiple_of(k * kc, kc), kc)
                prod = lax.dot_general(
                    scr[a, :, ks], bb[b, :, ks], (((1,), (1,)), ((), ())),
                    preferred_element_type=jnp.float32,
                )
                acc[t] += prod.reshape(vb, w, cols)
            each(depth // kc, kk)
            other = pl.ds(pl.multiple_of((1 - x) * half, half), half)
            xs[t] = acc[t, :, other, :].astype(jnp.bfloat16)
            xcopy(t).start()
        each(hi, mm, lo)

    def drain(lo, hi, b):
        def fin(a):
            t = a * SIDE + b
            xcopy(t).wait_recv()
            mine = pl.ds(pl.multiple_of(x * half, half), half)
            total = acc[t, :, mine, :] + xr[t].astype(jnp.float32)

            @pl.when(a == 0)
            def _():
                out[:, pl.ds(owned_c(0, b), 1), :, :] = total[:, None]

            @pl.when(a > 0)
            def _():
                zs[t] = total.astype(jnp.bfloat16)
                zcopy(t).start()
        each(hi, fin, lo)

    own_a.wait()
    screen(0)
    own_b.wait()
    a1.wait_recv()
    screen(1)
    group(0, 2, 0)

    def pass_a(k):
        a2(k).wait_recv()
        a3(k).start()

    def pass_b(k):
        b2(k).wait_recv()
        b3(k).start()

    def take_a():
        each(CHUNKS, lambda k: a3(k).wait_recv())
        screen(2)
        screen(3)

    @pl.when(end)
    def _():
        each(CHUNKS, pass_b)
        drain(0, 2, 0)
        b1.wait_recv()
        each(3, lambda b: group(0, 2, b), 1)
        each(3, lambda b: drain(0, 2, b), 1)
        each(CHUNKS, pass_a)
        take_a()
        each(3, lambda b: group(2, 4, b))
        each(3, lambda b: drain(2, 4, b))

    @pl.when(jnp.logical_not(end))
    def _():
        each(CHUNKS, pass_a)
        each(CHUNKS, lambda k: b2(k).wait_send())
        each(CHUNKS, lambda k: a2(k).start())
        drain(0, 2, 0)
        take_a()
        group(2, 4, 0)
        b1.wait_recv()
        group(0, 4, 1)
        drain(2, 4, 0)
        drain(0, 4, 1)
        each(CHUNKS, pass_b)
        group(0, 4, 2)
        drain(0, 4, 2)

    each(CHUNKS, lambda k: b3(k).wait_recv())
    group(0, 4, 3)
    drain(0, 4, 3)

    def land(t):
        zcopy(t).wait_recv()
        c = owned_c(t // SIDE, t % SIDE)
        out[:, pl.ds(c, 1), :, :] = zr[t].astype(jnp.float32)[:, None]
    each(SIDE * SIDE, land, SIDE)

    a1.wait_send()
    b1.wait_send()

    def sent(k):
        a2(k).wait_send()
        a3(k).wait_send()
        b3(k).wait_send()
    each(CHUNKS, sent)

    @pl.when(end)
    def _():
        each(CHUNKS, lambda k: b2(k).wait_send())
    each(SIDE * SIDE, lambda t: xcopy(t).wait_send())
    each(SIDE * SIDE, lambda t: zcopy(t).wait_send(), SIDE)


def grid_body(valence_pairs, conduction_pairs, screening):
    vb, w, depth = valence_pairs.shape
    bands, conduction, _ = conduction_pairs.shape
    cols = bands * conduction
    rows = vb * w
    half = w // lax.axis_size("pw")
    total_c = bands * lax.axis_size("pair")
    tiles = SIDE * SIDE
    dma = pltpu.SemaphoreType.DMA
    bf16 = jnp.bfloat16
    return pl.pallas_call(
        grid_kernel,
        out_shape=jax.ShapeDtypeStruct((vb, total_c, half, conduction), jnp.float32),
        in_specs=[
            pl.BlockSpec(memory_space=pl.ANY),
            pl.BlockSpec(memory_space=pl.ANY),
            pl.BlockSpec(memory_space=pltpu.VMEM),
        ],
        out_specs=pl.BlockSpec(memory_space=pltpu.VMEM),
        scratch_shapes=[
            pltpu.VMEM((SIDE, rows, depth), bf16),
            pltpu.VMEM((SIDE, rows, depth), bf16),
            pltpu.VMEM((SIDE, cols, depth), bf16),
            pltpu.VMEM((tiles, vb, w, cols), jnp.float32),
            pltpu.VMEM((tiles, vb, half, cols), bf16),
            pltpu.VMEM((tiles, vb, half, cols), bf16),
            pltpu.VMEM((tiles, vb, half, cols), bf16),
            pltpu.VMEM((tiles, vb, half, cols), bf16),
            dma((2,)),
            dma((1,)), dma((1,)),
            dma((CHUNKS,)), dma((CHUNKS,)), dma((CHUNKS,)), dma((CHUNKS,)),
            dma((1,)), dma((1,)),
            dma((CHUNKS,)), dma((CHUNKS,)), dma((CHUNKS,)), dma((CHUNKS,)),
            dma((tiles,)), dma((tiles,)), dma((tiles,)), dma((tiles,)),
        ],
        compiler_params=pltpu.CompilerParams(
            collective_id=0, has_side_effects=True, vmem_limit_bytes=56 * 1024 * 1024
        ),
    )(
        valence_pairs.reshape(rows, depth),
        conduction_pairs.reshape(cols, depth),
        screening.reshape(1, depth),
    )


def solution(mesh):
    placed = (P("pair", None, "pw"), P("pair", None, "pw"), P("pw"))
    squared = mesh.shape["pw"] == 2 and mesh.shape["pair"] == SIDE * SIDE

    def body(valence_pairs, conduction_pairs, screening):
        if squared and conduction_pairs.shape[0] == 1:
            return grid_body(valence_pairs, conduction_pairs, screening)
        return general_body(valence_pairs, conduction_pairs, screening)

    return jax.shard_map(
        body, mesh=mesh, in_specs=placed, out_specs=P("pair", None, "pw", None), check_vma=False
    )
```

```python
import functools

import jax
import jax.numpy as jnp
from jax import lax
from jax.experimental import pallas as pl
from jax.experimental.pallas import tpu as pltpu
from jax.sharding import PartitionSpec as P

MESH = pl.DeviceIdType.MESH
SIDE = 4
CHUNKS = 16


def contract(piece, flat_right, band_dev, conduction):
    first, second, width = piece.shape
    product = lax.dot_general(
        piece.reshape(first * second, width),
        flat_right,
        (((1,), (1,)), ((), ())),
        preferred_element_type=jnp.float32,
    )
    return product.reshape(first, second, band_dev, conduction)


def general_body(valence_pairs, conduction_pairs, screening):
    screened = (valence_pairs.astype(jnp.float32) * screening[None, None, :]).astype(jnp.bfloat16)
    band_dev, conduction, plane_dev = conduction_pairs.shape
    flat_local = conduction_pairs.reshape(band_dev * conduction, plane_dev)
    partial_value = contract(
        lax.all_gather(screened, "pair", axis=0, tiled=True), flat_local, band_dev, conduction
    )
    terms = lax.psum_scatter(partial_value, "pw", scatter_dimension=1, tiled=True)
    owned = lax.all_to_all(terms, "pair", split_axis=0, concat_axis=2, tiled=True)
    return owned.transpose(0, 2, 1, 3)


def flip(bit, by):
    return bit + by - 2 * bit * by


def grid_kernel(
    val, con, scr_row, out, raw, scr, bb, acc, xs, xr, zs, zr,
    loc, a1s, a1r, a2s, a2r, a3s, a3r, b1s, b1r, b2s, b2r, b3s, b3r, xss, xsr, zss, zsr,
):
    me, x = lax.axis_index("pair"), lax.axis_index("pw")
    core, y, zl, zh = me % 2, (me // 2) % 2, (me // 4) % 2, me // 8
    rows, depth = val.shape
    cols = con.shape[0]
    half = out.shape[2]
    step = rows // CHUNKS
    cstep = cols // CHUNKS

    def at(fc, fy, fl, fh):
        return (x, flip(core, fc) + 2 * flip(y, fy) + 4 * flip(zl, fl) + 8 * flip(zh, fh))

    def remote(src, dst, s, r, dev):
        return pltpu.make_async_remote_copy(
            src_ref=src, dst_ref=dst, send_sem=s, recv_sem=r, device_id=dev, device_id_type=MESH
        )

    def arows(k):
        return pl.ds(pl.multiple_of(k * step, step), step)

    def brows(k):
        return pl.ds(pl.multiple_of(k * cstep, cstep), cstep)

    sibling, beside, near, far = at(1, 0, 0, 0), at(0, 1, 0, 0), at(0, 0, 1, 0), at(0, 0, 0, 1)
    a1 = remote(val, raw.at[1], a1s.at[0], a1r.at[0], sibling)
    b1 = remote(con, bb.at[1], b1s.at[0], b1r.at[0], beside)

    def a2(k):
        return remote(val.at[arows(k)], raw.at[2, arows(k)], a2s.at[k], a2r.at[k], near)

    def b2(k):
        return remote(con.at[brows(k)], bb.at[2, brows(k)], b2s.at[k], b2r.at[k], far)

    def a3(k):
        return remote(raw.at[2, arows(k)], raw.at[3, arows(k)], a3s.at[k], a3r.at[k], sibling)

    def b3(k):
        return remote(bb.at[2, brows(k)], bb.at[3, brows(k)], b3s.at[k], b3r.at[k], beside)

    def xcopy(t):
        return remote(xs.at[t], xr.at[t], xss.at[t], xsr.at[t], (1 - x, me))

    def zcopy(t):
        a = t // SIDE
        return remote(zs.at[t], zr.at[t], zss.at[t], zsr.at[t], at(a % 2, 0, a // 2, 0))

    def each(n, fn, lo=0):
        def run(k, carry):
            fn(k)
            return carry
        lax.fori_loop(lo, n, run, 0)

    barrier = pltpu.get_barrier_semaphore()
    greeted = (sibling, beside, near, far, at(1, 0, 1, 0), (1 - x, me))
    for dev in greeted:
        pl.semaphore_signal(barrier, inc=1, device_id=dev, device_id_type=MESH)
    own_a = pltpu.make_async_copy(val, raw.at[0], loc.at[0])
    own_b = pltpu.make_async_copy(con, bb.at[0], loc.at[1])
    own_a.start()
    own_b.start()
    pl.semaphore_wait(barrier, len(greeted))

    end = zl == zh

    @pl.when(end)
    def _():
        each(CHUNKS, lambda k: a2(k).start())
        each(CHUNKS, lambda k: b2(k).start())

    @pl.when(jnp.logical_not(end))
    def _():
        each(CHUNKS, lambda k: b2(k).start())

    b1.start()
    a1.start()

    def screen(a):
        def part(i):
            r = pl.ds(pl.multiple_of(i * 16, 16), 16)
            scr[a, r, :] = (raw[a, r, :].astype(jnp.float32) * scr_row[...]).astype(jnp.bfloat16)
        each(rows // 16, part)

    vb, w = acc.shape[1], acc.shape[2]

    def owned_c(a, b):
        return flip(core, a % 2) + 2 * flip(y, b % 2) + 4 * flip(zl, a // 2) + 8 * flip(zh, b // 2)

    def group(lo, hi, b):
        def mm(a):
            t = a * SIDE + b
            prod = lax.dot_general(
                scr[a], bb[b], (((1,), (1,)), ((), ())), preferred_element_type=jnp.float32
            )
            acc[t] = prod.reshape(vb, w, cols)
            other = pl.ds(pl.multiple_of((1 - x) * half, half), half)
            xs[t] = acc[t, :, other, :].astype(jnp.bfloat16)
            xcopy(t).start()
        each(hi, mm, lo)

    def drain(lo, hi, b):
        def fin(a):
            t = a * SIDE + b
            xcopy(t).wait_recv()
            mine = pl.ds(pl.multiple_of(x * half, half), half)
            total = acc[t, :, mine, :] + xr[t].astype(jnp.float32)

            @pl.when(a == 0)
            def _():
                out[:, pl.ds(owned_c(0, b), 1), :, :] = total[:, None]

            @pl.when(a > 0)
            def _():
                zs[t] = total.astype(jnp.bfloat16)
                zcopy(t).start()
        each(hi, fin, lo)

    own_a.wait()
    screen(0)
    own_b.wait()
    a1.wait_recv()
    screen(1)
    group(0, 2, 0)

    def pass_a(k):
        a2(k).wait_recv()
        a3(k).start()

    def pass_b(k):
        b2(k).wait_recv()
        b3(k).start()

    def take_a():
        each(CHUNKS, lambda k: a3(k).wait_recv())
        screen(2)
        screen(3)

    @pl.when(end)
    def _():
        each(CHUNKS, pass_b)
        drain(0, 2, 0)
        b1.wait_recv()
        each(3, lambda b: group(0, 2, b), 1)
        each(3, lambda b: drain(0, 2, b), 1)
        each(CHUNKS, pass_a)
        take_a()
        each(3, lambda b: group(2, 4, b))
        each(3, lambda b: drain(2, 4, b))

    @pl.when(jnp.logical_not(end))
    def _():
        each(CHUNKS, pass_a)
        each(CHUNKS, lambda k: b2(k).wait_send())
        each(CHUNKS, lambda k: a2(k).start())
        drain(0, 2, 0)
        take_a()
        group(2, 4, 0)
        b1.wait_recv()
        group(0, 4, 1)
        drain(2, 4, 0)
        drain(0, 4, 1)
        each(CHUNKS, pass_b)
        group(0, 4, 2)
        drain(0, 4, 2)

    each(CHUNKS, lambda k: b3(k).wait_recv())
    group(0, 4, 3)
    drain(0, 4, 3)

    def land(t):
        zcopy(t).wait_recv()
        c = owned_c(t // SIDE, t % SIDE)
        out[:, pl.ds(c, 1), :, :] = zr[t].astype(jnp.float32)[:, None]
    each(SIDE * SIDE, land, SIDE)

    a1.wait_send()
    b1.wait_send()

    def sent(k):
        a2(k).wait_send()
        a3(k).wait_send()
        b3(k).wait_send()
    each(CHUNKS, sent)

    @pl.when(end)
    def _():
        each(CHUNKS, lambda k: b2(k).wait_send())
    each(SIDE * SIDE, lambda t: xcopy(t).wait_send())
    each(SIDE * SIDE, lambda t: zcopy(t).wait_send(), SIDE)


def grid_body(valence_pairs, conduction_pairs, screening):
    vb, w, depth = valence_pairs.shape
    bands, conduction, _ = conduction_pairs.shape
    cols = bands * conduction
    rows = vb * w
    half = w // lax.axis_size("pw")
    total_c = bands * lax.axis_size("pair")
    tiles = SIDE * SIDE
    dma = pltpu.SemaphoreType.DMA
    bf16 = jnp.bfloat16
    return pl.pallas_call(
        grid_kernel,
        out_shape=jax.ShapeDtypeStruct((vb, total_c, half, conduction), jnp.float32),
        in_specs=[
            pl.BlockSpec(memory_space=pl.ANY),
            pl.BlockSpec(memory_space=pl.ANY),
            pl.BlockSpec(memory_space=pltpu.VMEM),
        ],
        out_specs=pl.BlockSpec(memory_space=pltpu.VMEM),
        scratch_shapes=[
            pltpu.VMEM((SIDE, rows, depth), bf16),
            pltpu.VMEM((SIDE, rows, depth), bf16),
            pltpu.VMEM((SIDE, cols, depth), bf16),
            pltpu.VMEM((tiles, vb, w, cols), jnp.float32),
            pltpu.VMEM((tiles, vb, half, cols), bf16),
            pltpu.VMEM((tiles, vb, half, cols), bf16),
            pltpu.VMEM((tiles, vb, half, cols), bf16),
            pltpu.VMEM((tiles, vb, half, cols), bf16),
            dma((2,)),
            dma((1,)), dma((1,)),
            dma((CHUNKS,)), dma((CHUNKS,)), dma((CHUNKS,)), dma((CHUNKS,)),
            dma((1,)), dma((1,)),
            dma((CHUNKS,)), dma((CHUNKS,)), dma((CHUNKS,)), dma((CHUNKS,)),
            dma((tiles,)), dma((tiles,)), dma((tiles,)), dma((tiles,)),
        ],
        compiler_params=pltpu.CompilerParams(
            collective_id=0, has_side_effects=True, vmem_limit_bytes=56 * 1024 * 1024
        ),
    )(
        valence_pairs.reshape(rows, depth),
        conduction_pairs.reshape(cols, depth),
        screening.reshape(1, depth),
    )


def solution(mesh):
    placed = (P("pair", None, "pw"), P("pair", None, "pw"), P("pw"))
    squared = mesh.shape["pw"] == 2 and mesh.shape["pair"] == SIDE * SIDE

    def body(valence_pairs, conduction_pairs, screening):
        if squared and conduction_pairs.shape[0] == 1:
            return grid_body(valence_pairs, conduction_pairs, screening)
        return general_body(valence_pairs, conduction_pairs, screening)

    return jax.shard_map(
        body, mesh=mesh, in_specs=placed, out_specs=P("pair", None, "pw", None), check_vma=False
    )
```
